512 devices in a mesh: row: 16 (over z, y_lo), head: 32 (over x, y_hi, core).
Axes of the slice: x: 4, y: 8 (y_hi: 4, y_lo: 2; y = y_hi * 2 + y_lo), z: 8, core: 2. Of those that a mesh axis runs over, the one named last changes fastest.
Arguments:
- q_nope: bfloat16 [2048, 16384], P('row', 'head'), may hold values from -6 to 6
- q_rope: bfloat16 [2048, 8192], P('row', 'head'), may hold values from -192 to 192
- latent_keys: bfloat16 [512, 4096], P(None, 'row'), may hold values from -6 to 6
- rope_keys: bfloat16 [64, 4096], P(None, 'row'), may hold values from -8 to 8
- panel_block: int32 [16], replicated, may hold values from 0 to 63, as said below
- query_pos: int32 [2048], P('row'), may hold values from 1 to 16383
- w_uk: bfloat16 [128, 128, 512], P('head'), may hold values from -0.5 to 0.5
- w_uv: bfloat16 [128, 512, 128], P('head'), may hold values from -1 to 1
- w_out: bfloat16 [7168, 16384], P('row', 'head'), may hold values from -0.09375 to 0.09375
Outputs:
- attn_out: bfloat16 [2048, 7168], P(('row', 'head'))
The draws below stay inside these ranges and needn't reach their ends.
Inputs may be any that keep to these rules, and one draw needn't show every extreme that they name: `panel_block`: distinct block numbers; 0 and the largest allowed block are always among them.
All inputs are finite; a program needn't handle non-finite values.
Results may differ from the reference program's by a relative error of at most 0.025.
Values may be sent and summed in bfloat16 or wider, within the bound.
A program may use at most 64 MiB of HBM per device.

```python
import jax
import jax.numpy as jnp
from jax import lax

D = 7168
HEADS = 128
NOPE = 128
ROPE = 64
LATENT = 512
VHEAD = 128
PANEL = 256
QROWS = 2048
CACHE = 4096
N_ROW = 16


def draw_q_rope(key, part):
    sample = jax.random.truncated_normal(jax.random.fold_in(key, 17), -6.0, 6.0, (QROWS, HEADS * ROPE), jnp.float32)
    return sample.astype(jnp.bfloat16)


def draw_rope_keys(key, part):
    sample = jax.random.truncated_normal(jax.random.fold_in(key, 29), -6.0, 6.0, (ROPE, CACHE), jnp.float32)
    return sample.astype(jnp.bfloat16)


def draw_panel_block(key, part):
    middle = jax.random.permutation(jax.random.fold_in(key, 71), 4 * N_ROW - 2)[:N_ROW - 2] + 1
    ends = jnp.array([0, 4 * N_ROW - 1], jnp.int32)
    chosen = jnp.concatenate((ends, middle.astype(jnp.int32)))
    order = jax.random.permutation(jax.random.fold_in(key, 73), N_ROW)
    return chosen[order].astype(jnp.int32)


def set_ends(drawn, rng, smallest, top_value):
    shape = drawn.shape
    spot = [jax.random.randint(jax.random.fold_in(rng, axis), (), 0, shape[axis]) for axis in range(len(shape))]
    drawn = drawn.at[tuple(spot)].set(smallest)
    longest = shape.index(max(shape))
    spot[longest] = (spot[longest] + 1) % shape[longest]
    return drawn.at[tuple(spot)].set(top_value)


def steps_of(own_key, extent, pieces, smallest, largest):
    def one(dim, blocks):
        steps = jax.random.uniform(jax.random.fold_in(jax.random.fold_in(own_key, 6), dim), (blocks,), jnp.float32, smallest / len(pieces), largest / len(pieces))
        return jnp.repeat(jnp.exp(steps), extent[dim] // blocks).reshape((-1,) + (1,) * (len(extent) - dim - 1))

    loudness = one(*pieces[0])
    for cut in pieces[1:]:
        loudness = loudness * one(*cut)
    return loudness


def gaussian(stream_key, extent, width, bound, pieces=(), held_as=jnp.bfloat16):
    values = width * jax.random.normal(stream_key, extent, jnp.float32)
    if pieces:
        values = values * steps_of(stream_key, extent, pieces, -0.22, 0.18)
    return jnp.clip(values, -bound, bound).astype(held_as)


def setup_inputs(seed: int = 0) -> dict:
    streams_of = jax.random.split(jax.random.key(seed), 10)
    return {
        "q_nope": gaussian(streams_of[0], (QROWS, HEADS * NOPE), 1.0, 6.0, ((0, 16), (1, 32))),
        "q_rope": draw_q_rope(jax.random.fold_in(streams_of[9], 71), 0),
        "latent_keys": gaussian(streams_of[2], (LATENT, CACHE), 1.0, 6.0, ((1, 16),)),
        "rope_keys": draw_rope_keys(jax.random.fold_in(streams_of[9], 71), 0),
        "panel_block": draw_panel_block(jax.random.fold_in(streams_of[9], 71), 0),
        "query_pos": set_ends(jax.random.randint(streams_of[5], (QROWS,), 1, 4 * CACHE), jax.random.fold_in(streams_of[5], 1), 1, (4 * CACHE) - 1).astype(jnp.int32),
        "w_uk": gaussian(streams_of[6], (HEADS, NOPE, LATENT), NOPE ** -0.5, 0.5, ((0, 32),)),
        "w_uv": gaussian(streams_of[7], (HEADS, LATENT, VHEAD), (LATENT // 16) ** -0.5, 1.0, ((0, 32),)),
        "w_out": gaussian(streams_of[8], (D, HEADS * VHEAD), (HEADS * VHEAD // 4) ** -0.5, 0.09375, ((0, 16), (1, 32))),
    }


softmax_scale = 192.0 ** -0.5


def reference(q_nope, q_rope, latent_keys, rope_keys, panel_block, query_pos, w_uk, w_uv, w_out):
    columns = jnp.arange(CACHE, dtype=jnp.int32)
    key_pos = (panel_block[columns // PANEL] * PANEL + columns % PANEL).astype(jnp.int32)
    visible = key_pos[None, :] <= query_pos[:, None]
    nope_heads = jnp.transpose(q_nope.reshape(QROWS, HEADS, NOPE), (1, 0, 2))
    rope_heads = jnp.transpose(q_rope.reshape(QROWS, HEADS, ROPE), (1, 0, 2))

    def one_head(operands):
        query_nope, query_rope, absorb, expand = operands
        query_latent = jnp.dot(query_nope, absorb, preferred_element_type=jnp.float32).astype(jnp.bfloat16)
        scores = jnp.dot(query_latent, latent_keys, preferred_element_type=jnp.float32)
        scores = scores + jnp.dot(query_rope, rope_keys, preferred_element_type=jnp.float32)
        scores = jnp.where(visible, scores * softmax_scale, -jnp.inf)
        row_max = jnp.max(scores, axis=1, keepdims=True)
        weights = jnp.exp(scores - row_max)
        denominator = jnp.sum(weights, axis=1, keepdims=True)
        summed = jnp.dot(weights.astype(jnp.bfloat16), latent_keys.T, preferred_element_type=jnp.float32)
        mixed_latent = (summed / denominator).astype(jnp.bfloat16)
        return jnp.dot(mixed_latent, expand, preferred_element_type=jnp.float32).astype(jnp.bfloat16)

    head_values = lax.map(one_head, (nope_heads, rope_heads, w_uk, w_uv))
    values = jnp.transpose(head_values, (1, 0, 2)).reshape(QROWS, HEADS * VHEAD)
    return jnp.dot(values, w_out.T, preferred_element_type=jnp.float32).astype(jnp.bfloat16)
```

```python
import functools

import jax
import jax.numpy as jnp
from jax import lax
from jax.experimental import pallas as pl
from jax.experimental.pallas import tpu as pltpu
from jax.sharding import Mesh
from jax.sharding import PartitionSpec as P

NOPE = 128
ROPE = 64
LATENT = 512
VHEAD = 128
PANEL = 256
AXES = ("z", "ylo", "x", "yhi", "core")
ROW = ("z", "ylo")
HEAD = ("x", "yhi", "core")
MESH = pl.DeviceIdType.MESH
NZ, NX, NY = 8, 4, 4
DZ = (0, 1, 7, 2, 6, 3, 5, 4)
OFF = (0, -1, 1, -2, 2, -3, 3, 4)
LIMIT = ((4, 3), (3, 4))

softmax_scale = 192.0 ** (-0.5)


def mod(a, n):
    return lax.rem(a + n, n)


def remote(src, dst, send_sem, recv_sem, device):
    return pltpu.make_async_remote_copy(
        src_ref=src,
        dst_ref=dst,
        send_sem=send_sem,
        recv_sem=recv_sem,
        device_id=device,
        device_id_type=MESH,
    )


def meet(peers):
    barrier = pltpu.get_barrier_semaphore()
    for peer in peers:
        pl.semaphore_signal(barrier, inc=1, device_id=peer, device_id_type=MESH)
    pl.semaphore_wait(barrier, len(peers))


def gather_kernel(lat, rope, out, kv, send_sem, z_sem, x_sem, y_sem, c_sem, load_sem, out_sem):
    z, ylo, x, yhi, c = (lax.axis_index(a) for a in AXES)
    way = 1 - 2 * c
    here = z * 2 + ylo

    def piece(panel, half, part):
        return (panel * 2 + half) * 4 + part

    loads = []
    for half in range(2):
        lanes = pl.ds(128 * half, 128)
        for part in range(3):
            loads.append((lat.at[pl.ds(144 * part, 144), lanes], kv.at[piece(here, half, part)]))
        last = kv.at[piece(here, half, 3)]
        loads.append((lat.at[pl.ds(432, 80), lanes], last.at[pl.ds(0, 80)]))
        loads.append((rope.at[:, lanes], last.at[pl.ds(80, 64)]))
    loads = [pltpu.make_async_copy(s, d, load_sem.at[i]) for i, (s, d) in enumerate(loads)]
    for load in loads:
        load.start()
    y_up = {"ylo": 1 - ylo, "yhi": mod(yhi + ylo, NY)}
    y_down = {"ylo": 1 - ylo, "yhi": mod(yhi + ylo - 1, NY)}
    peers = [{"z": mod(z + d, NZ)} for d in range(1, NZ)]
    peers += [{"x": mod(x + 1, NX)}, {"x": mod(x - 1, NX)}, y_up, y_down, {"core": 1 - c}]
    meet(peers)
    for load in loads:
        load.wait()

    def copy_out(panel, half, slot):
        copy = pltpu.make_async_copy(
            kv.at[pl.ds(piece(panel, half, 0), 4)],
            out.at[:, :, pl.ds(pl.multiple_of(panel * PANEL + half * 128, 128), 128)],
            out_sem.at[slot],
        )
        copy.start()
        outs.append(copy)

    outs = []
    mine = kv.at[piece(here, c, x)]
    for d in (1, 7, 2, 6, 3, 5, 4):
        remote(mine, mine, send_sem.at[0], z_sem.at[DZ.index(d)], {"z": mod(z + d, NZ)}).start()

    def panel_of(k, low):
        return mod(z - DZ[k], NZ) * 2 + low

    def spread_y(k, part, turn):
        ref = kv.at[piece(panel_of(k, ylo), c, part)]
        to = {"ylo": 1 - ylo, "yhi": mod(yhi + ylo - lax.rem(part, 2), NY)}
        remote(ref, ref, send_sem.at[0], y_sem.at[k, turn], to).start()

    def spread_core(panel, part, slot):
        ref = kv.at[piece(panel, c, part)]
        remote(ref, ref, send_sem.at[0], c_sem.at[slot], {"core": 1 - c}).start()

    def spread_x(k, part, turn, step):
        ref = kv.at[piece(panel_of(k, ylo), c, part)]
        remote(ref, ref, send_sem.at[0], x_sem.at[k, turn], {"x": mod(x + step, NX)}).start()

    def arrived(ref, sem):
        remote(ref, ref, send_sem.at[0], sem, {"core": 1 - c}).wait_recv()

    parts = (x, mod(x - way, NX), mod(x + way, NX), mod(x + 2, NX))

    def stage_z(k):
        if k:
            arrived(kv.at[piece(panel_of(k, ylo), c, x)], z_sem.at[k])
            spread_x(k, x, 0, way)
            spread_x(k, x, 1, -way)
        spread_y(k, x, 0)
        if k:
            spread_core(panel_of(k, ylo), x, k)

    def stage_x(k, turns):
        for turn in turns:
            part = parts[turn + 1]
            if k:
                arrived(kv.at[piece(panel_of(k, ylo), c, part)], x_sem.at[k, turn])
            if k and turn == 0:
                spread_x(k, part, 2, way)
            spread_y(k, part, turn + 1)
            if k:
                spread_core(panel_of(k, ylo), part, k)
        if 2 in turns:
            copy_out(panel_of(k, ylo), c, 2 * k)

    def stage_y(k):
        panel = panel_of(k, 1 - ylo)
        for turn in range(4):
            arrived(kv.at[piece(panel, c, parts[turn])], y_sem.at[k, turn])
            spread_core(panel, parts[turn], 8 + k)
        copy_out(panel, c, 16 + 2 * k)

    def stage_core(k):
        panel = panel_of(k, ylo)
        if k:
            arrived(kv.at[pl.ds(piece(panel, 1 - c, 0), 4)], c_sem.at[k])
        copy_out(panel, 1 - c, 2 * k + 1)
        panel = panel_of(k, 1 - ylo)
        arrived(kv.at[pl.ds(piece(panel, 1 - c, 0), 4)], c_sem.at[8 + k])
        copy_out(panel, 1 - c, 16 + 2 * k + 1)

    for t in range(NZ + 4):
        if t < NZ:
            stage_z(t)
        if 0 <= t - 1 < NZ:
            stage_x(t - 1, (0, 1))
        if 0 <= t - 2 < NZ:
            stage_x(t - 2, (2,))
        if 0 <= t - 3 < NZ:
            stage_y(t - 3)
        if 0 <= t - 4 < NZ:
            stage_core(t - 4)
    for copy in outs:
        copy.wait()
    sent = kv.at[pl.ds(0, 7 + 21 + 32 + 28 + 32)]
    remote(sent, sent, send_sem.at[0], c_sem.at[0], {"core": 1 - c}).wait_send()


def gather_cache(lat, rope):
    return pl.pallas_call(
        gather_kernel,
        out_shape=jax.ShapeDtypeStruct((4, 144, 16 * PANEL), jnp.bfloat16),
        in_specs=[pl.BlockSpec(memory_space=pl.ANY)] * 2,
        out_specs=pl.BlockSpec(memory_space=pl.ANY),
        scratch_shapes=[
            pltpu.VMEM((128, 144, 128), jnp.bfloat16),
            pltpu.SemaphoreType.DMA((1,)),
            pltpu.SemaphoreType.DMA((8,)),
            pltpu.SemaphoreType.DMA((8, 3)),
            pltpu.SemaphoreType.DMA((8, 4)),
            pltpu.SemaphoreType.DMA((16,)),
            pltpu.SemaphoreType.DMA((10,)),
            pltpu.SemaphoreType.DMA((32,)),
        ],
        compiler_params=pltpu.CompilerParams(collective_id=0, has_side_effects=True),
        name="gather_cache",
    )(lat, rope)


def project_kernel(
    vals, w_near, w_far, out,
    vall, acc, cs, cr, xs, xr, xown, tb, ys, yr, yown, fs, fr,
    send_sem, ag_sem, c_sem, x_sem, y_sem, f_sem,
):
    z, ylo, x, yhi, c = (lax.axis_index(a) for a in AXES)
    partner = {"core": 1 - c}
    peers = [{"z": mod(z + d, NZ)} for d in range(1, NZ)]
    peers += [{"x": mod(x + d, NX)} for d in range(1, NX)]
    peers += [{"yhi": mod(yhi + d, NY)} for d in range(1, NY)]
    peers += [partner]
    meet(peers)
    steps = ({"z": mod(z + 1, NZ)}, {"z": mod(z - 1, NZ)})

    for sub in range(2):
        for side in range(2):
            remote(
                vals.at[sub], vall.at[2 * z + sub], send_sem.at[0], ag_sem.at[side, 0, sub], steps[side]
            ).start()

    def arrived(ref, sem):
        remote(ref, ref, send_sem.at[0], sem, partner).wait_recv()

    def land(m):
        dist = abs(OFF[m])
        source = mod(z + OFF[m], NZ)
        for sub in range(2):
            side = sub if dist == 4 else (0 if OFF[m] < 0 else 1)
            ref = vall.at[2 * source + sub]
            arrived(ref, ag_sem.at[side, dist - 1, sub])
            if dist + 1 <= LIMIT[side][sub]:
                remote(ref, ref, send_sem.at[0], ag_sem.at[side, dist, sub], steps[side]).start()
        return source

    def multiply(m):
        if m:
            source = land(m)
            rows = vall[pl.ds(2 * source, 2)].reshape(128, 512)
        else:
            rows = vals[...].reshape(128, 512)
        for j, w in enumerate((w_near, w_far)):
            product = lax.dot_general(
                rows, w[...], (((1,), (1,)), ((), ())), preferred_element_type=jnp.float32
            )
            acc[m, :, j] = product.reshape(2, 64, 448)
            cs[m, j] = acc[m, 1 - c, j].astype(jnp.bfloat16)
        remote(cs.at[m], cr.at[m], send_sem.at[1], c_sem.at[m], partner).start()

    def reduce_core(m):
        arrived(cr.at[m], c_sem.at[m])
        for d in (2, 1, 3, 0):
            at = pl.ds(pl.multiple_of(16 * mod(x + d, NX), 16), 16)
            for j in range(2):
                both = acc[m, c, j, at, :] + cr[m, j, at, :].astype(jnp.float32)
                if d:
                    xs[m, d - 1, j] = both.astype(jnp.bfloat16)
                else:
                    xown[m, j] = both
            if d:
                remote(
                    xs.at[m, d - 1], xr.at[m, d - 1], send_sem.at[2], x_sem.at[m, d - 1],
                    {"x": mod(x + d, NX)},
                ).start()

    def reduce_x(m):
        batch, k = divmod(m, 4)
        for d in range(3):
            arrived(xr.at[m, d], x_sem.at[m, d])
        for j in range(2):
            total = xown[m, j]
            for d in range(3):
                total = total + xr[m, d, j].astype(jnp.float32)
            tb[batch, j, 16 * k : 16 * k + 16, :] = total.astype(jnp.bfloat16)
        if k < 3:
            return
        row = lax.broadcasted_iota(jnp.int32, (16, 64), 0)
        column = lax.broadcasted_iota(jnp.int32, (16, 64), 1)
        first = (row // 4) * 16 + row % 4
        for d in (2, 1, 3, 0):
            to = mod(yhi + d, NY)
            pick = jnp.where(column == first + 4 * to, 1.0, 0.0).astype(jnp.bfloat16)
            for j in range(2):
                chosen = jnp.dot(pick, tb[batch, j], preferred_element_type=jnp.float32)
                if d:
                    ys[batch, d - 1, j] = chosen.astype(jnp.bfloat16)
                else:
                    yown[batch, j] = chosen
            if d:
                remote(
                    ys.at[batch, d - 1], yr.at[batch, d - 1], send_sem.at[3],
                    y_sem.at[batch, d - 1], {"yhi": to},
                ).start()

    def reduce_y(batch):
        for d in range(3):
            arrived(yr.at[batch, d], y_sem.at[batch, d])
        for j in range(2):
            total = yown[batch, j]
            for d in range(3):
                total = total + yr[batch, d, j].astype(jnp.float32)
            for k in range(4):
                rows = total[4 * k : 4 * k + 4].astype(jnp.bfloat16)
                if batch or k:
                    fs[4 * batch + k, j] = rows
                else:
                    fr[z, j] = rows
        for k in range(4):
            m = 4 * batch + k
            if m:
                remote(
                    fs.at[m], fr.at[z], send_sem.at[4], f_sem.at[m], {"z": mod(z + OFF[m], NZ)}
                ).start()

    for t in range(NZ + 2):
        if t < NZ:
            multiply(t)
        if 0 <= t - 1 < NZ:
            reduce_core(t - 1)
        if 0 <= t - 2 < NZ:
            reduce_x(t - 2)
        if t == 7:
            reduce_y(0)
    reduce_y(1)
    for m in range(1, NZ):
        arrived(fr.at[mod(z - OFF[m], NZ)], f_sem.at[m])
    for j in range(2):
        out[:, lax.rem(ylo + j, 2)] = fr[:, j]
    for ref, i in ((vall.at[pl.ds(0, 14)], 0), (cs, 1), (xs, 2), (ys, 3), (fs.at[pl.ds(1, 7)], 4)):
        remote(ref, ref, send_sem.at[i], c_sem.at[0], partner).wait_send()


def project(vals, w_near, w_far):
    bf, f32 = jnp.bfloat16, jnp.float32
    return pl.pallas_call(
        project_kernel,
        out_shape=jax.ShapeDtypeStruct((8, 2, 4, 448), bf),
        in_specs=[pl.BlockSpec(memory_space=pltpu.VMEM)] * 3,
        out_specs=pl.BlockSpec(memory_space=pltpu.VMEM),
        scratch_shapes=[
            pltpu.VMEM((16, 64, 512), bf),
            pltpu.VMEM((8, 2, 2, 64, 448), f32),
            pltpu.VMEM((8, 2, 64, 448), bf),
            pltpu.VMEM((8, 2, 64, 448), bf),
            pltpu.VMEM((8, 3, 2, 16, 448), bf),
            pltpu.VMEM((8, 3, 2, 16, 448), bf),
            pltpu.VMEM((8, 2, 16, 448), f32),
            pltpu.VMEM((2, 2, 64, 448), bf),
            pltpu.VMEM((2, 3, 2, 16, 448), bf),
            pltpu.VMEM((2, 3, 2, 16, 448), bf),
            pltpu.VMEM((2, 2, 16, 448), f32),
            pltpu.VMEM((8, 2, 4, 448), bf),
            pltpu.VMEM((8, 2, 4, 448), bf),
            pltpu.SemaphoreType.DMA((5,)),
            pltpu.SemaphoreType.DMA((2, 4, 2)),
            pltpu.SemaphoreType.DMA((8,)),
            pltpu.SemaphoreType.DMA((8, 3)),
            pltpu.SemaphoreType.DMA((2, 3)),
            pltpu.SemaphoreType.DMA((8,)),
        ],
        compiler_params=pltpu.CompilerParams(
            collective_id=1, has_side_effects=True, vmem_limit_bytes=48 << 20
        ),
        name="project",
    )(vals, w_near, w_far)


def on_device(q_nope, q_rope, latent_keys, rope_keys, panel_block, query_pos, w_uk, w_uv, w_out):
    row_count = q_nope.shape[0]
    head_count = w_uk.shape[0]
    nope_heads = q_nope.reshape(row_count, head_count, NOPE)
    query_latent = jnp.einsum(
        "rhn,hnl->hrl", nope_heads, w_uk, preferred_element_type=jnp.float32
    ).astype(jnp.bfloat16)
    query_latent = query_latent.reshape(head_count * row_count, LATENT)
    query_rope = jnp.transpose(q_rope.reshape(row_count, head_count, ROPE), (1, 0, 2)).reshape(
        head_count * row_count, ROPE
    )
    flat_pos = jnp.tile(query_pos, head_count)
    panel_count = panel_block.shape[0]
    panel_ids = jnp.arange(panel_count, dtype=jnp.int32)
    columns = jnp.arange(panel_count * PANEL, dtype=jnp.int32)
    owner = columns // PANEL
    block_of = jnp.sum(
        jnp.where(owner[:, None] == panel_ids[None, :], panel_block[None, :], 0), axis=1
    )
    key_pos = block_of * PANEL + columns % PANEL

    both = gather_cache(latent_keys, rope_keys).reshape(LATENT + ROPE, panel_count * PANEL)
    w_far = lax.ppermute(w_out, "ylo", [(0, 1), (1, 0)])
    latent_all, rope_all = both[:LATENT], both[LATENT:]
    scores = jnp.dot(query_latent, latent_all, preferred_element_type=jnp.float32)
    scores = scores + jnp.dot(query_rope, rope_all, preferred_element_type=jnp.float32)
    visible = key_pos[None, :] <= flat_pos[:, None]
    scores = jnp.where(visible, scores * softmax_scale, -jnp.inf)
    top = jnp.max(scores, axis=1)
    weights = jnp.exp(scores - top[:, None])
    denominator = jnp.sum(weights, axis=1)
    mixed = lax.dot_general(
        weights.astype(jnp.bfloat16),
        latent_all,
        (((1,), (1,)), ((), ())),
        preferred_element_type=jnp.float32,
    )
    mixed_latent = (
        (mixed / denominator[:, None])
        .astype(jnp.bfloat16)
        .reshape(head_count, row_count, LATENT)
    )
    values = jnp.einsum(
        "hrl,hlv->rhv", mixed_latent, w_uv, preferred_element_type=jnp.float32
    ).astype(jnp.bfloat16)
    values = values.reshape(NX, NY, 2, 4, head_count * VHEAD)
    values = jnp.transpose(values, (2, 0, 1, 3, 4)).reshape(2, 64, head_count * VHEAD)
    pieces = project(values, w_out, w_far)
    return jnp.transpose(pieces, (2, 0, 1, 3)).reshape(4, 7168)


def solution(mesh):
    finer = Mesh(mesh.devices.reshape(NZ, 2, NX, NY, 2), AXES)
    return jax.shard_map(
        on_device,
        mesh=finer,
        in_specs=(
            P(ROW, HEAD),
            P(ROW, HEAD),
            P(None, ROW),
            P(None, ROW),
            P(),
            P(ROW),
            P(HEAD, None, None),
            P(HEAD, None, None),
            P(ROW, HEAD),
        ),
        out_specs=P(ROW + HEAD, None),
        check_vma=False,
    )
```

```python
import jax
import jax.numpy as jnp
from jax import lax
from jax.experimental import pallas as pl
from jax.experimental.pallas import tpu as pltpu
from jax.sharding import Mesh
from jax.sharding import PartitionSpec as P

NOPE = 128
ROPE = 64
LATENT = 512
VHEAD = 128
PANEL = 256
KEYS = LATENT + ROPE
AXES = ("z", "ylo", "x", "yhi", "core")
ROW = ("z", "ylo")
HEAD = ("x", "yhi", "core")
MESH = pl.DeviceIdType.MESH
NZ, NX, NY = 8, 4, 4
HEADS, ROWS = 4, 128
SLICE = 448
DZ = (0, 1, 7, 2, 6, 3, 5, 4)
OFF = (0, -1, 1, -2, 2, -3, 3, 4)
SHIFTS = (3, 6, 9, 10)
SUBS = 4
LIMIT = ((4, 4, 3, 3), (3, 3, 4, 4))
ORDER = (
    ("a", 1), ("m", 0), ("a", 2), ("m", 1), ("m", 2), ("c", 0), ("a", 3), ("m", 3), ("m", 4),
    ("c", 1), ("c", 2), ("x", 0), ("a", 4), ("m", 5), ("m", 6), ("c", 3), ("c", 4), ("x", 1),
    ("x", 2), ("m", 7), ("c", 5), ("c", 6), ("x", 3), ("x", 4), ("c", 7), ("x", 5), ("x", 6),
    ("x", 7),
)
LOWEST = -1e30

softmax_scale = 192.0 ** (-0.5)


def mod(a, n):
    return lax.rem(a + n, n)


def remote(src, dst, send_sem, recv_sem, device):
    return pltpu.make_async_remote_copy(
        src_ref=src,
        dst_ref=dst,
        send_sem=send_sem,
        recv_sem=recv_sem,
        device_id=device,
        device_id_type=MESH,
    )


def meet(peers):
    barrier = pltpu.get_barrier_semaphore()
    for peer in peers:
        pl.semaphore_signal(barrier, inc=1, device_id=peer, device_id_type=MESH)
    pl.semaphore_wait(barrier, len(peers))


def kernel(
    q_nope, q_rope, lat, rope, blocks, query_pos, w_uk, w_uv, w_out, out,
    kv, nope, turned, expand, lift, wide, query, best, denom, mixed, vals,
    vall, acc, cs, cr, xs, xr, xown, fs, fr,
    load_sem, send_sem, z_sem, x_sem, y_sem, c_sem, w_sem,
    ag_sem, d_sem, r_sem, f_sem,
):
    z, ylo, x, yhi, c = (lax.axis_index(a) for a in AXES)
    bf, f32 = jnp.bfloat16, jnp.float32
    way = 1 - 2 * c
    here = z * 2 + ylo
    partner = {"core": 1 - c}

    def home(m, d):
        return {"z": mod(z + OFF[m], NZ), "yhi": mod(yhi + d, NY)}

    def piece(panel, half, part):
        return (panel * 2 + half) * 4 + part

    near = pl.ds(pl.multiple_of(SLICE * ylo, SLICE), SLICE)
    loads = []
    for half in range(2):
        lanes = pl.ds(128 * half, 128)
        for part in range(3):
            loads.append((lat.at[pl.ds(144 * part, 144), lanes], kv.at[piece(here, half, part)]))
        last = kv.at[piece(here, half, 3)]
        loads.append((lat.at[pl.ds(432, 80), lanes], last.at[pl.ds(0, 80)]))
        loads.append((rope.at[:, lanes], last.at[pl.ds(80, 64)]))
    loads += [(q_nope, nope), (q_rope, turned), (w_uk, lift), (w_uv, expand), (w_out, wide.at[near])]
    loads = [pltpu.make_async_copy(s, d, load_sem.at[i]) for i, (s, d) in enumerate(loads)]
    for load in loads:
        load.start()
    y_up = {"ylo": 1 - ylo, "yhi": mod(yhi + ylo, NY)}
    y_down = {"ylo": 1 - ylo, "yhi": mod(yhi + ylo - 1, NY)}
    peers = [home(m, d) for m in range(NZ) for d in range(NY) if m or d]
    peers += [{"x": mod(x + d, NX)} for d in range(1, NX)]
    peers += [y_up, y_down, partner]
    meet(peers)
    for load in loads[:10]:
        load.wait()

    def arrived(ref, sem):
        remote(ref, ref, send_sem.at[0], sem, partner).wait_recv()

    mine = kv.at[piece(here, c, x)]
    for d in (1, 7, 2, 6, 3, 5, 4):
        remote(mine, mine, send_sem.at[0], z_sem.at[DZ.index(d)], {"z": mod(z + d, NZ)}).start()

    def panel_of(k, low):
        return mod(z - DZ[k], NZ) * 2 + low

    def spread_y(k, part, turn):
        ref = kv.at[piece(panel_of(k, ylo), c, part)]
        to = {"ylo": 1 - ylo, "yhi": mod(yhi + ylo - lax.rem(part, 2), NY)}
        remote(ref, ref, send_sem.at[0], y_sem.at[k, turn], to).start()

    def spread_core(panel, part, slot):
        ref = kv.at[piece(panel, c, part)]
        remote(ref, ref, send_sem.at[0], c_sem.at[slot], partner).start()

    def spread_x(k, part, turn, step):
        ref = kv.at[piece(panel_of(k, ylo), c, part)]
        remote(ref, ref, send_sem.at[0], x_sem.at[k, turn], {"x": mod(x + step, NX)}).start()

    parts = (x, mod(x - way, NX), mod(x + way, NX), mod(x + 2, NX))

    def stage_z(k):
        if k:
            arrived(kv.at[piece(panel_of(k, ylo), c, x)], z_sem.at[k])
            spread_x(k, x, 0, way)
            spread_x(k, x, 1, -way)
        spread_y(k, x, 0)
        if k:
            spread_core(panel_of(k, ylo), x, k)

    def stage_x(k, turns):
        for turn in turns:
            part = parts[turn + 1]
            if k:
                arrived(kv.at[piece(panel_of(k, ylo), c, part)], x_sem.at[k, turn])
            if k and turn == 0:
                spread_x(k, part, 2, way)
            spread_y(k, part, turn + 1)
            if k:
                spread_core(panel_of(k, ylo), part, k)

    def stage_y(k):
        panel = panel_of(k, 1 - ylo)
        for turn in range(4):
            arrived(kv.at[piece(panel, c, parts[turn])], y_sem.at[k, turn])
            spread_core(panel, parts[turn], 8 + k)

    def stage_core(k):
        if k:
            arrived(kv.at[pl.ds(piece(panel_of(k, ylo), 1 - c, 0), 4)], c_sem.at[k])
        arrived(kv.at[pl.ds(piece(panel_of(k, 1 - ylo), 1 - c, 0), 4)], c_sem.at[8 + k])

    across = lax.broadcasted_iota(jnp.int32, (ROWS, ROWS), 1)
    down = lax.broadcasted_iota(jnp.int32, (ROWS, ROWS), 0)
    row_pos = jnp.sum(
        jnp.where(across == down, query_pos[...].astype(f32), 0.0), axis=1, keepdims=True
    )

    def absorb():
        for load in loads[10:13]:
            load.wait()
        for h in range(HEADS):
            lifted = jnp.dot(
                nope[:, NOPE * h : NOPE * h + NOPE], lift[h], preferred_element_type=f32
            )
            at = slice(ROWS * h, ROWS * h + ROWS)
            query[at, :LATENT] = lifted.astype(bf)
            query[at, LATENT:] = turned[:, ROPE * h : ROPE * h + ROPE]

    def attend(k):
        panels = (panel_of(k, ylo), panel_of(k, 1 - ylo))
        lane = lax.broadcasted_iota(jnp.int32, (1, 128), 1)
        spots = jnp.concatenate(
            [blocks[p] * PANEL + 128 * half + lane for p in panels for half in range(2)], axis=1
        ).astype(f32)

        def one_head(h, carry):
            at = pl.ds(pl.multiple_of(ROWS * h, ROWS), ROWS)
            keys = jnp.concatenate(
                [
                    kv[pl.ds(piece(p, half, 0), 4)].reshape(KEYS, 128)
                    for p in panels
                    for half in range(2)
                ],
                axis=1,
            )
            scores = jnp.dot(query[at, :], keys, preferred_element_type=f32)
            scores = jnp.where(spots <= row_pos, scores * softmax_scale, -jnp.inf)
            top = jnp.max(scores, axis=1, keepdims=True)
            if k:
                before = best[at, :1]
                top = jnp.maximum(before, top)
                shrink = jnp.exp(before - top)
            else:
                top = jnp.maximum(top, LOWEST)
            weights = jnp.exp(scores - top)
            total = jnp.sum(weights, axis=1, keepdims=True)
            update = lax.dot_general(
                weights.astype(bf), keys[:LATENT], (((1,), (1,)), ((), ())),
                preferred_element_type=f32,
            )
            if k:
                total = total + denom[at, :1] * shrink
                update = update + mixed[at, :] * shrink
            best[at, :] = jnp.broadcast_to(top, (ROWS, 128))
            denom[at, :] = jnp.broadcast_to(total, (ROWS, 128))
            mixed[at, :] = update
            return carry

        lax.fori_loop(0, HEADS, one_head, 0)

    for t in range(NZ + SHIFTS[-1]):
        if t < NZ:
            stage_z(t)
        if t == 0:
            absorb()
        if 0 <= t - SHIFTS[0] < NZ:
            stage_x(t - SHIFTS[0], (0, 1))
        if 0 <= t - SHIFTS[1] < NZ:
            stage_x(t - SHIFTS[1], (2,))
        if t == SHIFTS[1] + NZ - 1:
            loads[14].wait()
            remote(
                wide.at[near], wide.at[near], send_sem.at[5], w_sem.at[0], {"ylo": 1 - ylo}
            ).start()
        if 0 <= t - SHIFTS[2] < NZ:
            stage_y(t - SHIFTS[2])
        if 0 <= t - SHIFTS[3] < NZ:
            stage_core(t - SHIFTS[3])
            attend(t - SHIFTS[3])

    loads[13].wait()
    source = ((down % 64) // 4) * 8 + (down // 64) * 4 + down % 4
    order = jnp.where(across == source, 1.0, 0.0).astype(bf)
    for h in range(HEADS):
        at = slice(ROWS * h, ROWS * h + ROWS)
        latent = (mixed[at, :] / denom[at, :1]).astype(bf)
        head = jnp.dot(latent, expand[h], preferred_element_type=f32).astype(bf)
        head = jnp.dot(order, head, preferred_element_type=f32).astype(bf)
        vals[:, :, VHEAD * h : VHEAD * h + VHEAD] = head.reshape(SUBS, ROWS // SUBS, VHEAD)

    steps = ({"z": mod(z + 1, NZ)}, {"z": mod(z - 1, NZ)})

    for sub in range(SUBS):
        for side in range(2):
            remote(
                vals.at[sub], vall.at[SUBS * z + sub], send_sem.at[1], ag_sem.at[side, 0, sub],
                steps[side],
            ).start()

    def land(dist):
        for sub in range(SUBS):
            for side in range(2):
                if dist > LIMIT[side][sub]:
                    continue
                source = mod(z + (dist if side else -dist), NZ)
                ref = vall.at[SUBS * source + sub]
                arrived(ref, ag_sem.at[side, dist - 1, sub])
                if dist + 1 <= LIMIT[side][sub]:
                    remote(
                        ref, ref, send_sem.at[1], ag_sem.at[side, dist, sub], steps[side]
                    ).start()

    def multiply(m):
        if m:
            rows = vall[pl.ds(SUBS * mod(z + OFF[m], NZ), SUBS)].reshape(128, 512)
        else:
            rows = vals[...].reshape(128, 512)
        product = lax.dot_general(
            rows, wide[...], (((1,), (1,)), ((), ())), preferred_element_type=f32
        )
        acc[m] = product.reshape(2, 64, 2 * SLICE)
        cs[m] = acc[m, 1 - c].astype(bf)
        remote(cs.at[m], cr.at[m], send_sem.at[2], d_sem.at[m], partner).start()

    def reduce_core(m):
        arrived(cr.at[m], d_sem.at[m])
        for d in (2, 1, 3, 0):
            at = pl.ds(pl.multiple_of(16 * mod(x + d, NX), 16), 16)
            both = acc[m, c, at, :] + cr[m, at, :].astype(f32)
            if d:
                xs[m, d - 1] = both.astype(bf)
            else:
                xown[m] = both
            if d:
                remote(
                    xs.at[m, d - 1], xr.at[m, d - 1], send_sem.at[3], r_sem.at[m, d - 1],
                    {"x": mod(x + d, NX)},
                ).start()

    def reduce_x(m):
        for d in range(3):
            arrived(xr.at[m, d], r_sem.at[m, d])
        total = xown[m]
        for d in range(3):
            total = total + xr[m, d].astype(f32)
        for y in range(NY):
            fs[NY * m + y] = total[4 * y : 4 * y + 4].astype(bf)
        for d in (2, 1, 3, 0):
            ref = fs.at[NY * m + mod(yhi + d, NY)]
            if m or d:
                remote(ref, fr.at[m, d], send_sem.at[4], f_sem.at[m, d], home(m, d)).start()
            else:
                fr[0, 0] = fs[yhi]

    far = pl.ds(pl.multiple_of(SLICE * (1 - ylo), SLICE), SLICE)
    for step in ORDER:
        if step == ("m", 0):
            arrived(wide.at[far], w_sem.at[0])
        {"a": land, "m": multiply, "c": reduce_core, "x": reduce_x}[step[0]](step[1])
    for m in range(NZ):
        for d in range(NY):
            if m or d:
                arrived(fr.at[m, d], f_sem.at[m, d])
        total = fr[m, 0].astype(f32)
        for d in range(1, NY):
            total = total + fr[m, d].astype(f32)
        out[mod(z - OFF[m], NZ)] = total.astype(bf)
    pieces = kv.at[pl.ds(0, 7 + 21 + 32 + 28 + 32)]
    sent = (pieces, vall.at[pl.ds(0, 7 * SUBS)], cs, xs, fs.at[pl.ds(0, 31)], wide.at[near])
    for i, ref in enumerate(sent):
        remote(ref, ref, send_sem.at[i], w_sem.at[0], partner).wait_send()


def attention(*operands):
    bf, f32 = jnp.bfloat16, jnp.float32
    anywhere = pl.BlockSpec(memory_space=pl.ANY)
    vmem = pl.BlockSpec(memory_space=pltpu.VMEM)
    smem = pl.BlockSpec(memory_space=pltpu.SMEM)
    return pl.pallas_call(
        kernel,
        out_shape=jax.ShapeDtypeStruct((8, 4, 2 * SLICE), bf),
        in_specs=[anywhere] * 4 + [smem, vmem] + [anywhere] * 3,
        out_specs=vmem,
        scratch_shapes=[
            pltpu.VMEM((128, 144, 128), bf),
            pltpu.VMEM((ROWS, HEADS * NOPE), bf),
            pltpu.VMEM((ROWS, HEADS * ROPE), bf),
            pltpu.VMEM((HEADS, LATENT, VHEAD), bf),
            pltpu.VMEM((HEADS, NOPE, LATENT), bf),
            pltpu.VMEM((2 * SLICE, HEADS * VHEAD), bf),
            pltpu.VMEM((HEADS * ROWS, KEYS), bf),
            pltpu.VMEM((HEADS * ROWS, 128), f32),
            pltpu.VMEM((HEADS * ROWS, 128), f32),
            pltpu.VMEM((HEADS * ROWS, LATENT), f32),
            pltpu.VMEM((SUBS, ROWS // SUBS, HEADS * VHEAD), bf),
            pltpu.VMEM((NZ * SUBS, ROWS // SUBS, HEADS * VHEAD), bf),
            pltpu.VMEM((8, 2, 64, 2 * SLICE), f32),
            pltpu.VMEM((8, 64, 2 * SLICE), bf),
            pltpu.VMEM((8, 64, 2 * SLICE), bf),
            pltpu.VMEM((8, 3, 16, 2 * SLICE), bf),
            pltpu.VMEM((8, 3, 16, 2 * SLICE), bf),
            pltpu.VMEM((8, 16, 2 * SLICE), f32),
            pltpu.VMEM((32, 4, 2 * SLICE), bf),
            pltpu.VMEM((8, 4, 4, 2 * SLICE), bf),
            pltpu.SemaphoreType.DMA((15,)),
            pltpu.SemaphoreType.DMA((6,)),
            pltpu.SemaphoreType.DMA((8,)),
            pltpu.SemaphoreType.DMA((8, 3)),
            pltpu.SemaphoreType.DMA((8, 4)),
            pltpu.SemaphoreType.DMA((16,)),
            pltpu.SemaphoreType.DMA((1,)),
            pltpu.SemaphoreType.DMA((2, 4, SUBS)),
            pltpu.SemaphoreType.DMA((8,)),
            pltpu.SemaphoreType.DMA((8, 3)),
            pltpu.SemaphoreType.DMA((8, 4)),
        ],
        compiler_params=pltpu.CompilerParams(
            collective_id=0, has_side_effects=True, vmem_limit_bytes=56 << 20
        ),
        name="attention",
    )(*operands)


def on_device(q_nope, q_rope, latent_keys, rope_keys, panel_block, query_pos, w_uk, w_uv, w_out):
    pieces = attention(
        q_nope, q_rope, latent_keys, rope_keys, panel_block, query_pos.reshape(1, ROWS),
        w_uk, w_uv, w_out,
    )
    return jnp.transpose(pieces, (1, 0, 2)).reshape(4, NZ * 2 * SLICE)


def solution(mesh):
    finer = Mesh(mesh.devices.reshape(NZ, 2, NX, NY, 2), AXES)
    return jax.shard_map(
        on_device,
        mesh=finer,
        in_specs=(
            P(ROW, HEAD),
            P(ROW, HEAD),
            P(None, ROW),
            P(None, ROW),
            P(),
            P(ROW),
            P(HEAD, None, None),
            P(HEAD, None, None),
            P(ROW, HEAD),
        ),
        out_specs=P(ROW + HEAD, None),
        check_vma=False,
    )
```

```python
import jax
import jax.numpy as jnp
from jax import lax
from jax.experimental import pallas as pl
from jax.experimental.pallas import tpu as pltpu
from jax.sharding import Mesh
from jax.sharding import PartitionSpec as P

NOPE = 128
ROPE = 64
LATENT = 512
VHEAD = 128
PANEL = 256
KEYS = LATENT + ROPE
AXES = ("z", "ylo", "x", "yhi", "core")
ROW = ("z", "ylo")
HEAD = ("x", "yhi", "core")
MESH = pl.DeviceIdType.MESH
NZ, NX, NY = 8, 4, 4
HEADS, ROWS = 4, 128
SLICE = 448
DZ = (0, 1, 7, 2, 6, 3, 5, 4)
OFF = (0, -1, 1, -2, 2, -3, 3, 4)
SHIFTS = (3, 5, 7, 8)
SHARES = (8, 9, 10, 11)
BLOCK = 256
SUBS = 4
LIMIT = ((4, 4, 3, 3), (3, 3, 4, 4))
ORDER = (
    ("a", 1), ("m", 0), ("a", 2), ("m", 1), ("m", 2), ("c", 0), ("a", 3), ("m", 3), ("m", 4),
    ("c", 1), ("c", 2), ("x", 0), ("a", 4), ("m", 5), ("m", 6), ("c", 3), ("c", 4), ("x", 1),
    ("x", 2), ("m", 7), ("c", 5), ("c", 6), ("x", 3), ("x", 4), ("c", 7), ("x", 5), ("x", 6),
    ("x", 7),
)
LOWEST = -1e30

softmax_scale = 192.0 ** (-0.5)


def mod(a, n):
    return lax.rem(a + n, n)


def remote(src, dst, send_sem, recv_sem, device):
    return pltpu.make_async_remote_copy(
        src_ref=src,
        dst_ref=dst,
        send_sem=send_sem,
        recv_sem=recv_sem,
        device_id=device,
        device_id_type=MESH,
    )


def meet(peers):
    barrier = pltpu.get_barrier_semaphore()
    for peer in peers:
        pl.semaphore_signal(barrier, inc=1, device_id=peer, device_id_type=MESH)
    pl.semaphore_wait(barrier, len(peers))


def kernel(
    q_nope, q_rope, lat, rope, blocks, query_pos, w_uk, w_uv, w_out, out,
    kv, nope, turned, expand, lift, wide, query, best, denom, mixed, vals,
    vall, acc, cs, cr, xs, xr, xown, fs, fr,
    load_sem, send_sem, z_sem, x_sem, y_sem, c_sem, w_sem,
    ag_sem, d_sem, r_sem, f_sem,
):
    z, ylo, x, yhi, c = (lax.axis_index(a) for a in AXES)
    bf, f32 = jnp.bfloat16, jnp.float32
    way = 1 - 2 * c
    here = z * 2 + ylo
    partner = {"core": 1 - c}

    def home(m, d):
        return {"z": mod(z + OFF[m], NZ), "yhi": mod(yhi + d, NY)}

    def piece(panel, half, part):
        return (panel * 2 + half) * 4 + part

    near = pl.ds(pl.multiple_of(SLICE * ylo, SLICE), SLICE)
    loads = []
    for half in range(2):
        lanes = pl.ds(128 * half, 128)
        for part in range(3):
            loads.append((lat.at[pl.ds(144 * part, 144), lanes], kv.at[piece(here, half, part)]))
        last = kv.at[piece(here, half, 3)]
        loads.append((lat.at[pl.ds(432, 80), lanes], last.at[pl.ds(0, 80)]))
        loads.append((rope.at[:, lanes], last.at[pl.ds(80, 64)]))
    loads += [(q_nope, nope), (q_rope, turned), (w_uk, lift), (w_uv, expand), (w_out, wide.at[near])]
    loads = [pltpu.make_async_copy(s, d, load_sem.at[i]) for i, (s, d) in enumerate(loads)]
    for load in loads:
        load.start()
    y_up = {"ylo": 1 - ylo, "yhi": mod(yhi + ylo, NY)}
    y_down = {"ylo": 1 - ylo, "yhi": mod(yhi + ylo - 1, NY)}
    peers = [home(m, d) for m in range(NZ) for d in range(NY) if m or d]
    peers += [{"x": mod(x + d, NX)} for d in range(1, NX)]
    peers += [y_up, y_down, partner]
    meet(peers)
    for load in loads[:10]:
        load.wait()

    def arrived(ref, sem):
        remote(ref, ref, send_sem.at[0], sem, partner).wait_recv()

    mine = kv.at[piece(here, c, x)]
    for d in (1, 7, 2, 6, 3, 5, 4):
        remote(mine, mine, send_sem.at[0], z_sem.at[DZ.index(d)], {"z": mod(z + d, NZ)}).start()

    def panel_of(k, low):
        return mod(z - DZ[k], NZ) * 2 + low

    def spread_y(k, part, turn):
        ref = kv.at[piece(panel_of(k, ylo), c, part)]
        to = {"ylo": 1 - ylo, "yhi": mod(yhi + ylo - lax.rem(part, 2), NY)}
        remote(ref, ref, send_sem.at[0], y_sem.at[k, turn], to).start()

    def spread_core(panel, part, slot):
        ref = kv.at[piece(panel, c, part)]
        remote(ref, ref, send_sem.at[0], c_sem.at[slot], partner).start()

    def spread_x(k, part, turn, step):
        ref = kv.at[piece(panel_of(k, ylo), c, part)]
        remote(ref, ref, send_sem.at[0], x_sem.at[k, turn], {"x": mod(x + step, NX)}).start()

    parts = (x, mod(x - way, NX), mod(x + way, NX), mod(x + 2, NX))

    def stage_z(k):
        if k:
            arrived(kv.at[piece(panel_of(k, ylo), c, x)], z_sem.at[k])
            spread_x(k, x, 0, way)
            spread_x(k, x, 1, -way)
        spread_y(k, x, 0)
        if k:
            spread_core(panel_of(k, ylo), x, k)

    def stage_x(k, turns):
        for turn in turns:
            part = parts[turn + 1]
            if k:
                arrived(kv.at[piece(panel_of(k, ylo), c, part)], x_sem.at[k, turn])
            if k and turn == 0:
                spread_x(k, part, 2, way)
            spread_y(k, part, turn + 1)
            if k:
                spread_core(panel_of(k, ylo), part, k)

    def stage_y(k):
        panel = panel_of(k, 1 - ylo)
        for turn in range(4):
            arrived(kv.at[piece(panel, c, parts[turn])], y_sem.at[k, turn])
            spread_core(panel, parts[turn], 8 + k)

    def stage_core(k):
        if k:
            arrived(kv.at[pl.ds(piece(panel_of(k, ylo), 1 - c, 0), 4)], c_sem.at[k])
        arrived(kv.at[pl.ds(piece(panel_of(k, 1 - ylo), 1 - c, 0), 4)], c_sem.at[8 + k])

    def share(quarter):
        ref = wide.at[pl.ds(pl.multiple_of(SLICE * ylo + 112 * quarter, 16), 112)]
        remote(ref, ref, send_sem.at[5], w_sem.at[quarter], {"ylo": 1 - ylo}).start()

    across = lax.broadcasted_iota(jnp.int32, (ROWS, ROWS), 1)
    down = lax.broadcasted_iota(jnp.int32, (ROWS, ROWS), 0)
    row_pos = jnp.sum(
        jnp.where(across == down, query_pos[...].astype(f32), 0.0), axis=1, keepdims=True
    )

    rows_pos = jnp.concatenate([row_pos] * (BLOCK // ROWS), axis=0)

    def absorb():
        for load in loads[10:13]:
            load.wait()
        for h in range(HEADS):
            lifted = jnp.dot(
                nope[:, NOPE * h : NOPE * h + NOPE], lift[h], preferred_element_type=f32
            )
            at = slice(ROWS * h, ROWS * h + ROWS)
            query[at, :LATENT] = lifted.astype(bf)
            query[at, LATENT:] = turned[:, ROPE * h : ROPE * h + ROPE]

    def attend(k):
        panels = (panel_of(k, ylo), panel_of(k, 1 - ylo))
        lane = lax.broadcasted_iota(jnp.int32, (1, 128), 1)
        spots = jnp.concatenate(
            [blocks[p] * PANEL + 128 * half + lane for p in panels for half in range(2)], axis=1
        ).astype(f32)

        def one_block(b, carry):
            at = pl.ds(pl.multiple_of(BLOCK * b, BLOCK), BLOCK)
            keys = jnp.concatenate(
                [
                    kv[pl.ds(piece(p, half, 0), 4)].reshape(KEYS, 128)
                    for p in panels
                    for half in range(2)
                ],
                axis=1,
            )
            scores = jnp.dot(query[at, :], keys, preferred_element_type=f32)
            scores = jnp.where(spots <= rows_pos, scores * softmax_scale, -jnp.inf)
            top = jnp.max(scores, axis=1, keepdims=True)
            if k:
                before = best[at, :1]
                top = jnp.maximum(before, top)
                shrink = jnp.exp(before - top)
            else:
                top = jnp.maximum(top, LOWEST)
            weights = jnp.exp(scores - top)
            total = jnp.sum(weights, axis=1, keepdims=True)
            update = lax.dot_general(
                weights.astype(bf), keys[:LATENT], (((1,), (1,)), ((), ())),
                preferred_element_type=f32,
            )
            if k:
                total = total + denom[at, :1] * shrink
                update = update + mixed[at, :] * shrink
            best[at, :] = jnp.broadcast_to(top, (BLOCK, 128))
            denom[at, :] = jnp.broadcast_to(total, (BLOCK, 128))
            mixed[at, :] = update
            return carry

        lax.fori_loop(0, HEADS * ROWS // BLOCK, one_block, 0)

    for t in range(NZ + SHIFTS[-1]):
        if t < NZ:
            stage_z(t)
        if t == 0:
            absorb()
            loads[14].wait()
        if 0 <= t - SHIFTS[0] < NZ:
            stage_x(t - SHIFTS[0], (0, 1))
        if 0 <= t - SHIFTS[1] < NZ:
            stage_x(t - SHIFTS[1], (2,))
        if t in SHARES:
            share(SHARES.index(t))
        if 0 <= t - SHIFTS[2] < NZ:
            stage_y(t - SHIFTS[2])
        if 0 <= t - SHIFTS[3] < NZ:
            stage_core(t - SHIFTS[3])
            attend(t - SHIFTS[3])

    loads[13].wait()
    source = ((down % 64) // 4) * 8 + (down // 64) * 4 + down % 4
    order = jnp.where(across == source, 1.0, 0.0).astype(bf)
    for h in range(HEADS):
        at = slice(ROWS * h, ROWS * h + ROWS)
        latent = (mixed[at, :] / denom[at, :1]).astype(bf)
        head = jnp.dot(latent, expand[h], preferred_element_type=f32).astype(bf)
        head = jnp.dot(order, head, preferred_element_type=f32).astype(bf)
        vals[:, :, VHEAD * h : VHEAD * h + VHEAD] = head.reshape(SUBS, ROWS // SUBS, VHEAD)

    steps = ({"z": mod(z + 1, NZ)}, {"z": mod(z - 1, NZ)})

    for sub in range(SUBS):
        for side in range(2):
            remote(
                vals.at[sub], vall.at[SUBS * z + sub], send_sem.at[1], ag_sem.at[side, 0, sub],
                steps[side],
            ).start()

    def land(dist):
        for sub in range(SUBS):
            for side in range(2):
                if dist > LIMIT[side][sub]:
                    continue
                source = mod(z + (dist if side else -dist), NZ)
                ref = vall.at[SUBS * source + sub]
                arrived(ref, ag_sem.at[side, dist - 1, sub])
                if dist + 1 <= LIMIT[side][sub]:
                    remote(
                        ref, ref, send_sem.at[1], ag_sem.at[side, dist, sub], steps[side]
                    ).start()

    def multiply(m):
        if m:
            rows = vall[pl.ds(SUBS * mod(z + OFF[m], NZ), SUBS)].reshape(128, 512)
        else:
            rows = vals[...].reshape(128, 512)
        product = lax.dot_general(
            rows, wide[...], (((1,), (1,)), ((), ())), preferred_element_type=f32
        )
        acc[m] = product.reshape(2, 64, 2 * SLICE)
        cs[m] = acc[m, 1 - c].astype(bf)
        remote(cs.at[m], cr.at[m], send_sem.at[2], d_sem.at[m], partner).start()

    def reduce_core(m):
        arrived(cr.at[m], d_sem.at[m])
        for d in (2, 1, 3, 0):
            at = pl.ds(pl.multiple_of(16 * mod(x + d, NX), 16), 16)
            both = acc[m, c, at, :] + cr[m, at, :].astype(f32)
            if d:
                xs[m, d - 1] = both.astype(bf)
            else:
                xown[m] = both
            if d:
                remote(
                    xs.at[m, d - 1], xr.at[m, d - 1], send_sem.at[3], r_sem.at[m, d - 1],
                    {"x": mod(x + d, NX)},
                ).start()

    def reduce_x(m):
        for d in range(3):
            arrived(xr.at[m, d], r_sem.at[m, d])
        total = xown[m]
        for d in range(3):
            total = total + xr[m, d].astype(f32)
        for y in range(NY):
            fs[NY * m + y] = total[4 * y : 4 * y + 4].astype(bf)
        for d in (2, 1, 3, 0):
            ref = fs.at[NY * m + mod(yhi + d, NY)]
            if m or d:
                remote(ref, fr.at[m, d], send_sem.at[4], f_sem.at[m, d], home(m, d)).start()
            else:
                fr[0, 0] = fs[yhi]

    for step in ORDER:
        if step == ("m", 0):
            for quarter in range(4):
                away = pl.multiple_of(SLICE * (1 - ylo) + 112 * quarter, 16)
                arrived(wide.at[pl.ds(away, 112)], w_sem.at[quarter])
        {"a": land, "m": multiply, "c": reduce_core, "x": reduce_x}[step[0]](step[1])
    for m in range(NZ):
        for d in range(NY):
            if m or d:
                arrived(fr.at[m, d], f_sem.at[m, d])
        total = fr[m, 0].astype(f32)
        for d in range(1, NY):
            total = total + fr[m, d].astype(f32)
        at = pl.multiple_of(2 * SLICE * mod(z - OFF[m], NZ), 2 * SLICE)
        out[:, pl.ds(at, 2 * SLICE)] = total.astype(bf)
    pieces = kv.at[pl.ds(0, 7 + 21 + 32 + 28 + 32)]
    sent = (pieces, vall.at[pl.ds(0, 7 * SUBS)], cs, xs, fs.at[pl.ds(0, 31)], wide.at[near])
    for i, ref in enumerate(sent):
        remote(ref, ref, send_sem.at[i], w_sem.at[0], partner).wait_send()


def attention(*operands):
    bf, f32 = jnp.bfloat16, jnp.float32
    anywhere = pl.BlockSpec(memory_space=pl.ANY)
    vmem = pl.BlockSpec(memory_space=pltpu.VMEM)
    smem = pl.BlockSpec(memory_space=pltpu.SMEM)
    return pl.pallas_call(
        kernel,
        out_shape=jax.ShapeDtypeStruct((4, NZ * 2 * SLICE), bf),
        in_specs=[anywhere] * 4 + [smem, vmem] + [anywhere] * 3,
        out_specs=vmem,
        scratch_shapes=[
            pltpu.VMEM((128, 144, 128), bf),
            pltpu.VMEM((ROWS, HEADS * NOPE), bf),
            pltpu.VMEM((ROWS, HEADS * ROPE), bf),
            pltpu.VMEM((HEADS, LATENT, VHEAD), bf),
            pltpu.VMEM((HEADS, NOPE, LATENT), bf),
            pltpu.VMEM((2 * SLICE, HEADS * VHEAD), bf),
            pltpu.VMEM((HEADS * ROWS, KEYS), bf),
            pltpu.VMEM((HEADS * ROWS, 128), f32),
            pltpu.VMEM((HEADS * ROWS, 128), f32),
            pltpu.VMEM((HEADS * ROWS, LATENT), f32),
            pltpu.VMEM((SUBS, ROWS // SUBS, HEADS * VHEAD), bf),
            pltpu.VMEM((NZ * SUBS, ROWS // SUBS, HEADS * VHEAD), bf),
            pltpu.VMEM((8, 2, 64, 2 * SLICE), f32),
            pltpu.VMEM((8, 64, 2 * SLICE), bf),
            pltpu.VMEM((8, 64, 2 * SLICE), bf),
            pltpu.VMEM((8, 3, 16, 2 * SLICE), bf),
            pltpu.VMEM((8, 3, 16, 2 * SLICE), bf),
            pltpu.VMEM((8, 16, 2 * SLICE), f32),
            pltpu.VMEM((32, 4, 2 * SLICE), bf),
            pltpu.VMEM((8, 4, 4, 2 * SLICE), bf),
            pltpu.SemaphoreType.DMA((15,)),
            pltpu.SemaphoreType.DMA((6,)),
            pltpu.SemaphoreType.DMA((8,)),
            pltpu.SemaphoreType.DMA((8, 3)),
            pltpu.SemaphoreType.DMA((8, 4)),
            pltpu.SemaphoreType.DMA((16,)),
            pltpu.SemaphoreType.DMA((4,)),
            pltpu.SemaphoreType.DMA((2, 4, SUBS)),
            pltpu.SemaphoreType.DMA((8,)),
            pltpu.SemaphoreType.DMA((8, 3)),
            pltpu.SemaphoreType.DMA((8, 4)),
        ],
        compiler_params=pltpu.CompilerParams(
            collective_id=0, has_side_effects=True, vmem_limit_bytes=56 << 20
        ),
        name="attention",
    )(*operands)


def on_device(q_nope, q_rope, latent_keys, rope_keys, panel_block, query_pos, w_uk, w_uv, w_out):
    return attention(
        q_nope, q_rope, latent_keys, rope_keys, panel_block, query_pos.reshape(1, ROWS),
        w_uk, w_uv, w_out,
    )


def solution(mesh):
    finer = Mesh(mesh.devices.reshape(NZ, 2, NX, NY, 2), AXES)
    return jax.shard_map(
        on_device,
        mesh=finer,
        in_specs=(
            P(ROW, HEAD),
            P(ROW, HEAD),
            P(None, ROW),
            P(None, ROW),
            P(),
            P(ROW),
            P(HEAD, None, None),
            P(HEAD, None, None),
            P(ROW, HEAD),
        ),
        out_specs=P(ROW + HEAD, None),
        check_vma=False,
    )
```

```python
import jax
import jax.numpy as jnp
from jax import lax
from jax.experimental import pallas as pl
from jax.experimental.pallas import tpu as pltpu
from jax.sharding import Mesh
from jax.sharding import PartitionSpec as P

NOPE = 128
ROPE = 64
LATENT = 512
VHEAD = 128
PANEL = 256
KEYS = LATENT + ROPE
AXES = ("z", "ylo", "x", "yhi", "core")
ROW = ("z", "ylo")
HEAD = ("x", "yhi", "core")
MESH = pl.DeviceIdType.MESH
NZ, NX, NY = 8, 4, 4
HEADS, ROWS = 4, 128
SLICE = 448
DZ = (0, 1, 7, 2, 6, 3, 5, 4)
OFF = (0, -1, 1, -2, 2, -3, 3, 4)
SHIFTS = (3, 5, 7, 8)
SHARES = (10, 11, 12, 13)
BLOCK = 256
SUBS = 4
LIMIT = ((4, 4, 3, 3), (3, 3, 4, 4))
ORDER = (
    ("a", 1), ("m", 0), ("a", 2), ("m", 1), ("m", 2), ("c", 0), ("a", 3), ("m", 3), ("m", 4),
    ("c", 1), ("c", 2), ("x", 0), ("a", 4), ("m", 5), ("m", 6), ("c", 3), ("c", 4), ("x", 1),
    ("x", 2), ("m", 7), ("c", 5), ("c", 6), ("x", 3), ("x", 4), ("c", 7), ("x", 5), ("x", 6),
    ("x", 7),
)
LOWEST = -1e30

softmax_scale = 192.0 ** (-0.5)


def mod(a, n):
    return lax.rem(a + n, n)


def remote(src, dst, send_sem, recv_sem, device):
    return pltpu.make_async_remote_copy(
        src_ref=src,
        dst_ref=dst,
        send_sem=send_sem,
        recv_sem=recv_sem,
        device_id=device,
        device_id_type=MESH,
    )


def meet(peers):
    barrier = pltpu.get_barrier_semaphore()
    for peer in peers:
        pl.semaphore_signal(barrier, inc=1, device_id=peer, device_id_type=MESH)
    pl.semaphore_wait(barrier, len(peers))


def kernel(
    q_nope, q_rope, lat, rope, blocks, query_pos, w_uk, w_uv, w_out, out,
    kv, nope, turned, expand, lift, wide, query, best, denom, mixed, vals,
    vall, acc, cs, cr, xs, xr, xown, fs, fr,
    load_sem, send_sem, z_sem, x_sem, y_sem, c_sem, w_sem,
    ag_sem, d_sem, r_sem, f_sem,
):
    z, ylo, x, yhi, c = (lax.axis_index(a) for a in AXES)
    bf, f32 = jnp.bfloat16, jnp.float32
    way = 1 - 2 * c
    here = z * 2 + ylo
    partner = {"core": 1 - c}

    def home(m, d):
        return {"z": mod(z + OFF[m], NZ), "yhi": mod(yhi + d, NY)}

    def piece(panel, half, part):
        return (panel * 2 + half) * 4 + part

    near = pl.ds(pl.multiple_of(SLICE * ylo, SLICE), SLICE)
    loads = []
    for half in range(2):
        lanes = pl.ds(128 * half, 128)
        for part in range(3):
            loads.append((lat.at[pl.ds(144 * part, 144), lanes], kv.at[piece(here, half, part)]))
        last = kv.at[piece(here, half, 3)]
        loads.append((lat.at[pl.ds(432, 80), lanes], last.at[pl.ds(0, 80)]))
        loads.append((rope.at[:, lanes], last.at[pl.ds(80, 64)]))
    loads += [(q_nope, nope), (q_rope, turned), (w_uk, lift), (w_uv, expand), (w_out, wide.at[near])]
    loads = [pltpu.make_async_copy(s, d, load_sem.at[i]) for i, (s, d) in enumerate(loads)]
    for load in loads:
        load.start()
    y_up = {"ylo": 1 - ylo, "yhi": mod(yhi + ylo, NY)}
    y_down = {"ylo": 1 - ylo, "yhi": mod(yhi + ylo - 1, NY)}
    peers = [home(m, d) for m in range(NZ) for d in range(NY) if m or d]
    peers += [{"x": mod(x + d, NX)} for d in range(1, NX)]
    peers += [y_up, y_down, partner]
    meet(peers)
    for load in loads[:10]:
        load.wait()

    def arrived(ref, sem):
        remote(ref, ref, send_sem.at[0], sem, partner).wait_recv()

    mine = kv.at[piece(here, c, x)]
    for d in (1, 7, 2, 6, 3, 5, 4):
        remote(mine, mine, send_sem.at[0], z_sem.at[DZ.index(d)], {"z": mod(z + d, NZ)}).start()

    def panel_of(k, low):
        return mod(z - DZ[k], NZ) * 2 + low

    def spread_y(k, part, turn):
        ref = kv.at[piece(panel_of(k, ylo), c, part)]
        to = {"ylo": 1 - ylo, "yhi": mod(yhi + ylo - lax.rem(part, 2), NY)}
        remote(ref, ref, send_sem.at[0], y_sem.at[k, turn], to).start()

    def spread_core(panel, part, slot):
        ref = kv.at[piece(panel, c, part)]
        remote(ref, ref, send_sem.at[0], c_sem.at[slot], partner).start()

    def spread_x(k, part, turn, step):
        ref = kv.at[piece(panel_of(k, ylo), c, part)]
        remote(ref, ref, send_sem.at[0], x_sem.at[k, turn], {"x": mod(x + step, NX)}).start()

    parts = (x, mod(x - way, NX), mod(x + way, NX), mod(x + 2, NX))

    def stage_z(k):
        if k:
            arrived(kv.at[piece(panel_of(k, ylo), c, x)], z_sem.at[k])
            spread_x(k, x, 0, way)
            spread_x(k, x, 1, -way)
        spread_y(k, x, 0)
        if k:
            spread_core(panel_of(k, ylo), x, k)

    def stage_x(k, turns):
        for turn in turns:
            part = parts[turn + 1]
            if k:
                arrived(kv.at[piece(panel_of(k, ylo), c, part)], x_sem.at[k, turn])
            if k and turn == 0:
                spread_x(k, part, 2, way)
            spread_y(k, part, turn + 1)
            if k:
                spread_core(panel_of(k, ylo), part, k)

    def stage_y(k):
        panel = panel_of(k, 1 - ylo)
        for turn in range(4):
            arrived(kv.at[piece(panel, c, parts[turn])], y_sem.at[k, turn])
            spread_core(panel, parts[turn], 8 + k)

    def stage_core(k):
        if k:
            arrived(kv.at[pl.ds(piece(panel_of(k, ylo), 1 - c, 0), 4)], c_sem.at[k])
        arrived(kv.at[pl.ds(piece(panel_of(k, 1 - ylo), 1 - c, 0), 4)], c_sem.at[8 + k])

    def share(quarter):
        ref = wide.at[pl.ds(pl.multiple_of(SLICE * ylo + 112 * quarter, 16), 112)]
        remote(ref, ref, send_sem.at[5], w_sem.at[quarter], {"ylo": 1 - ylo}).start()

    across = lax.broadcasted_iota(jnp.int32, (ROWS, ROWS), 1)
    down = lax.broadcasted_iota(jnp.int32, (ROWS, ROWS), 0)
    row_pos = jnp.sum(
        jnp.where(across == down, query_pos[...].astype(f32), 0.0), axis=1, keepdims=True
    )

    rows_pos = jnp.concatenate([row_pos] * (BLOCK // ROWS), axis=0)

    def absorb():
        for load in loads[10:13]:
            load.wait()
        for h in range(HEADS):
            lifted = jnp.dot(
                nope[:, NOPE * h : NOPE * h + NOPE], lift[h], preferred_element_type=f32
            )
            at = slice(ROWS * h, ROWS * h + ROWS)
            query[at, :LATENT] = lifted.astype(bf)
            query[at, LATENT:] = turned[:, ROPE * h : ROPE * h + ROPE]

    def attend(k):
        panels = (panel_of(k, ylo), panel_of(k, 1 - ylo))
        lane = lax.broadcasted_iota(jnp.int32, (1, 128), 1)
        spots = jnp.concatenate(
            [blocks[p] * PANEL + 128 * half + lane for p in panels for half in range(2)], axis=1
        ).astype(f32)

        def one_block(b, carry):
            at = pl.ds(pl.multiple_of(BLOCK * b, BLOCK), BLOCK)
            keys = jnp.concatenate(
                [
                    kv[pl.ds(piece(p, half, 0), 4)].reshape(KEYS, 128)
                    for p in panels
                    for half in range(2)
                ],
                axis=1,
            )
            scores = jnp.dot(query[at, :], keys, preferred_element_type=f32)
            scores = jnp.where(spots <= rows_pos, scores * softmax_scale, -jnp.inf)
            top = jnp.max(scores, axis=1, keepdims=True)
            if k:
                before = best[at, :1]
                top = jnp.maximum(before, top)
                shrink = jnp.exp(before - top)
            else:
                top = jnp.maximum(top, LOWEST)
            weights = jnp.exp(scores - top)
            total = jnp.sum(weights, axis=1, keepdims=True)
            update = lax.dot_general(
                weights.astype(bf), keys[:LATENT], (((1,), (1,)), ((), ())),
                preferred_element_type=f32,
            )
            if k:
                total = total + denom[at, :1] * shrink
                update = update + mixed[at, :] * shrink
            best[at, :] = jnp.broadcast_to(top, (BLOCK, 128))
            denom[at, :] = jnp.broadcast_to(total, (BLOCK, 128))
            mixed[at, :] = update
            return carry

        lax.fori_loop(0, HEADS * ROWS // BLOCK, one_block, 0)

    for t in range(NZ + SHIFTS[-1]):
        if t < NZ:
            stage_z(t)
        if t == 2:
            absorb()
            loads[14].wait()
        if 0 <= t - SHIFTS[0] < NZ:
            stage_x(t - SHIFTS[0], (0, 1))
        if 0 <= t - SHIFTS[1] < NZ:
            stage_x(t - SHIFTS[1], (2,))
        if t in SHARES:
            share(SHARES.index(t))
        if 0 <= t - SHIFTS[2] < NZ:
            stage_y(t - SHIFTS[2])
        if 0 <= t - SHIFTS[3] < NZ:
            stage_core(t - SHIFTS[3])
            attend(t - SHIFTS[3])

    steps = ({"z": mod(z + 1, NZ)}, {"z": mod(z - 1, NZ)})

    def publish(sub):
        for side in range(2):
            remote(
                vals.at[sub], vall.at[SUBS * z + sub], send_sem.at[1], ag_sem.at[side, 0, sub],
                steps[side],
            ).start()

    loads[13].wait()
    source = ((down % 64) // 4) * 8 + (down // 64) * 4 + down % 4
    order = jnp.where(across == source, 1.0, 0.0).astype(bf)
    for h in (0, 2, 1, 3):
        at = slice(ROWS * h, ROWS * h + ROWS)
        latent = (mixed[at, :] / denom[at, :1]).astype(bf)
        head = jnp.dot(latent, expand[h], preferred_element_type=f32).astype(bf)
        head = jnp.dot(order, head, preferred_element_type=f32).astype(bf)
        vals[h] = head
        publish(h)

    def land(dist):
        for sub in (0, 2, 1, 3):
            for side in range(2):
                if dist > LIMIT[side][sub]:
                    continue
                source = mod(z + (dist if side else -dist), NZ)
                ref = vall.at[SUBS * source + sub]
                arrived(ref, ag_sem.at[side, dist - 1, sub])
                if dist + 1 <= LIMIT[side][sub]:
                    remote(
                        ref, ref, send_sem.at[1], ag_sem.at[side, dist, sub], steps[side]
                    ).start()

    def multiply(m):
        held = [vall.at[SUBS * mod(z + OFF[m], NZ) + h] if m else vals.at[h] for h in range(HEADS)]
        rows = jnp.concatenate([ref[...] for ref in held], axis=1)
        product = lax.dot_general(
            rows, wide[...], (((1,), (1,)), ((), ())), preferred_element_type=f32
        )
        acc[m] = product.reshape(2, 64, 2 * SLICE)
        cs[m] = acc[m, 1 - c].astype(bf)
        remote(cs.at[m], cr.at[m], send_sem.at[2], d_sem.at[m], partner).start()

    def reduce_core(m):
        arrived(cr.at[m], d_sem.at[m])
        for d in (2, 1, 3, 0):
            at = pl.ds(pl.multiple_of(16 * mod(x + d, NX), 16), 16)
            both = acc[m, c, at, :] + cr[m, at, :].astype(f32)
            if d:
                xs[m, d - 1] = both.astype(bf)
            else:
                xown[m] = both
            if d:
                remote(
                    xs.at[m, d - 1], xr.at[m, d - 1], send_sem.at[3], r_sem.at[m, d - 1],
                    {"x": mod(x + d, NX)},
                ).start()

    def reduce_x(m):
        for d in range(3):
            arrived(xr.at[m, d], r_sem.at[m, d])
        total = xown[m]
        for d in range(3):
            total = total + xr[m, d].astype(f32)
        for y in range(NY):
            fs[NY * m + y] = total[4 * y : 4 * y + 4].astype(bf)
        for d in (2, 1, 3, 0):
            ref = fs.at[NY * m + mod(yhi + d, NY)]
            if m or d:
                remote(ref, fr.at[m, d], send_sem.at[4], f_sem.at[m, d], home(m, d)).start()
            else:
                fr[0, 0] = fs[yhi]

    for step in ORDER:
        if step == ("m", 0):
            for quarter in range(4):
                away = pl.multiple_of(SLICE * (1 - ylo) + 112 * quarter, 16)
                arrived(wide.at[pl.ds(away, 112)], w_sem.at[quarter])
        {"a": land, "m": multiply, "c": reduce_core, "x": reduce_x}[step[0]](step[1])
    for m in range(NZ):
        for d in range(NY):
            if m or d:
                arrived(fr.at[m, d], f_sem.at[m, d])
        total = fr[m, 0].astype(f32)
        for d in range(1, NY):
            total = total + fr[m, d].astype(f32)
        at = pl.multiple_of(2 * SLICE * mod(z - OFF[m], NZ), 2 * SLICE)
        out[:, pl.ds(at, 2 * SLICE)] = total.astype(bf)
    pieces = kv.at[pl.ds(0, 7 + 21 + 32 + 28 + 32)]
    sent = (pieces, vall.at[pl.ds(0, 7 * SUBS)], cs, xs, fs.at[pl.ds(0, 31)], wide.at[near])
    for i, ref in enumerate(sent):
        remote(ref, ref, send_sem.at[i], w_sem.at[0], partner).wait_send()


def attention(*operands):
    bf, f32 = jnp.bfloat16, jnp.float32
    anywhere = pl.BlockSpec(memory_space=pl.ANY)
    vmem = pl.BlockSpec(memory_space=pltpu.VMEM)
    smem = pl.BlockSpec(memory_space=pltpu.SMEM)
    return pl.pallas_call(
        kernel,
        out_shape=jax.ShapeDtypeStruct((4, NZ * 2 * SLICE), bf),
        in_specs=[anywhere] * 4 + [smem, vmem] + [anywhere] * 3,
        out_specs=vmem,
        scratch_shapes=[
            pltpu.VMEM((128, 144, 128), bf),
            pltpu.VMEM((ROWS, HEADS * NOPE), bf),
            pltpu.VMEM((ROWS, HEADS * ROPE), bf),
            pltpu.VMEM((HEADS, LATENT, VHEAD), bf),
            pltpu.VMEM((HEADS, NOPE, LATENT), bf),
            pltpu.VMEM((2 * SLICE, HEADS * VHEAD), bf),
            pltpu.VMEM((HEADS * ROWS, KEYS), bf),
            pltpu.VMEM((HEADS * ROWS, 128), f32),
            pltpu.VMEM((HEADS * ROWS, 128), f32),
            pltpu.VMEM((HEADS * ROWS, LATENT), f32),
            pltpu.VMEM((SUBS, ROWS, VHEAD), bf),
            pltpu.VMEM((NZ * SUBS, ROWS, VHEAD), bf),
            pltpu.VMEM((8, 2, 64, 2 * SLICE), f32),
            pltpu.VMEM((8, 64, 2 * SLICE), bf),
            pltpu.VMEM((8, 64, 2 * SLICE), bf),
            pltpu.VMEM((8, 3, 16, 2 * SLICE), bf),
            pltpu.VMEM((8, 3, 16, 2 * SLICE), bf),
            pltpu.VMEM((8, 16, 2 * SLICE), f32),
            pltpu.VMEM((32, 4, 2 * SLICE), bf),
            pltpu.VMEM((8, 4, 4, 2 * SLICE), bf),
            pltpu.SemaphoreType.DMA((15,)),
            pltpu.SemaphoreType.DMA((6,)),
            pltpu.SemaphoreType.DMA((8,)),
            pltpu.SemaphoreType.DMA((8, 3)),
            pltpu.SemaphoreType.DMA((8, 4)),
            pltpu.SemaphoreType.DMA((16,)),
            pltpu.SemaphoreType.DMA((4,)),
            pltpu.SemaphoreType.DMA((2, 4, SUBS)),
            pltpu.SemaphoreType.DMA((8,)),
            pltpu.SemaphoreType.DMA((8, 3)),
            pltpu.SemaphoreType.DMA((8, 4)),
        ],
        compiler_params=pltpu.CompilerParams(
            collective_id=0, has_side_effects=True, vmem_limit_bytes=56 << 20
        ),
        name="attention",
    )(*operands)


def on_device(q_nope, q_rope, latent_keys, rope_keys, panel_block, query_pos, w_uk, w_uv, w_out):
    return attention(
        q_nope, q_rope, latent_keys, rope_keys, panel_block, query_pos.reshape(1, ROWS),
        w_uk, w_uv, w_out,
    )


def solution(mesh):
    finer = Mesh(mesh.devices.reshape(NZ, 2, NX, NY, 2), AXES)
    return jax.shard_map(
        on_device,
        mesh=finer,
        in_specs=(
            P(ROW, HEAD),
            P(ROW, HEAD),
            P(None, ROW),
            P(None, ROW),
            P(),
            P(ROW),
            P(HEAD, None, None),
            P(HEAD, None, None),
            P(ROW, HEAD),
        ),
        out_specs=P(ROW + HEAD, None),
        check_vma=False,
    )
```

```python
import jax
import jax.numpy as jnp
from jax import lax
from jax.experimental import pallas as pl
from jax.experimental.pallas import tpu as pltpu
from jax.sharding import Mesh
from jax.sharding import PartitionSpec as P

NOPE = 128
ROPE = 64
LATENT = 512
VHEAD = 128
PANEL = 256
KEYS = LATENT + ROPE
AXES = ("z", "ylo", "x", "yhi", "core")
ROW = ("z", "ylo")
HEAD = ("x", "yhi", "core")
MESH = pl.DeviceIdType.MESH
NZ, NX, NY = 8, 4, 4
HEADS, ROWS = 4, 128
SLICE = 448
DZ = (0, 1, 7, 2, 6, 3, 5, 4)
OFF = (0, -1, 1, -2, 2, -3, 3, 4)
SHIFTS = (3, 5, 7, 8)
SHARES = (10, 11, 12, 13)
BLOCK = 256
SUBS = 4
LIMIT = ((4, 4, 3, 3), (3, 3, 4, 4))
ORDER = (
    ("a", 1), ("m", 0), ("a", 2), ("m", 1), ("m", 2), ("c", 0), ("a", 3), ("m", 3), ("m", 4),
    ("c", 1), ("c", 2), ("x", 0), ("a", 4), ("m", 5), ("m", 6), ("c", 3), ("c", 4), ("x", 1),
    ("x", 2), ("m", 7), ("c", 5), ("c", 6), ("x", 3), ("x", 4), ("c", 7), ("x", 5), ("x", 6),
    ("x", 7),
)
LOWEST = -1e30

softmax_scale = 192.0 ** (-0.5)


def mod(a, n):
    return lax.rem(a + n, n)


def remote(src, dst, send_sem, recv_sem, device):
    return pltpu.make_async_remote_copy(
        src_ref=src,
        dst_ref=dst,
        send_sem=send_sem,
        recv_sem=recv_sem,
        device_id=device,
        device_id_type=MESH,
    )


def meet(peers):
    barrier = pltpu.get_barrier_semaphore()
    for peer in peers:
        pl.semaphore_signal(barrier, inc=1, device_id=peer, device_id_type=MESH)
    pl.semaphore_wait(barrier, len(peers))


def kernel(
    q_nope, q_rope, lat, rope, blocks, query_pos, w_uk, w_uv, w_out, out,
    kv, nope, turned, expand, lift, wide, query, best, denom, mixed, vals,
    vall, acc, cs, cr, xs, xr, xown, fs, fr,
    load_sem, send_sem, z_sem, x_sem, y_sem, c_sem, w_sem,
    ag_sem, d_sem, r_sem, f_sem,
):
    z, ylo, x, yhi, c = (lax.axis_index(a) for a in AXES)
    bf, f32 = jnp.bfloat16, jnp.float32
    way = 1 - 2 * c
    here = z * 2 + ylo
    partner = {"core": 1 - c}

    def home(m, d):
        return {"z": mod(z + OFF[m], NZ), "yhi": mod(yhi + d, NY)}

    def piece(panel, half, part):
        return (panel * 2 + half) * 4 + part

    near = pl.ds(pl.multiple_of(SLICE * ylo, SLICE), SLICE)
    loads = []
    for half in range(2):
        lanes = pl.ds(128 * half, 128)
        for part in range(3):
            loads.append((lat.at[pl.ds(144 * part, 144), lanes], kv.at[piece(here, half, part)]))
        last = kv.at[piece(here, half, 3)]
        loads.append((lat.at[pl.ds(432, 80), lanes], last.at[pl.ds(0, 80)]))
        loads.append((rope.at[:, lanes], last.at[pl.ds(80, 64)]))
    loads += [(q_nope, nope), (q_rope, turned), (w_uk, lift), (w_uv, expand), (w_out, wide.at[near])]
    loads = [pltpu.make_async_copy(s, d, load_sem.at[i]) for i, (s, d) in enumerate(loads)]
    for load in loads:
        load.start()
    y_up = {"ylo": 1 - ylo, "yhi": mod(yhi + ylo, NY)}
    y_down = {"ylo": 1 - ylo, "yhi": mod(yhi + ylo - 1, NY)}
    peers = [home(m, d) for m in range(NZ) for d in range(NY) if m or d]
    peers += [{"x": mod(x + d, NX)} for d in range(1, NX)]
    peers += [y_up, y_down, partner]
    meet(peers)
    for load in loads[:10]:
        load.wait()

    def arrived(ref, sem):
        remote(ref, ref, send_sem.at[0], sem, partner).wait_recv()

    mine = kv.at[piece(here, c, x)]
    for d in (1, 7, 2, 6, 3, 5, 4):
        remote(mine, mine, send_sem.at[0], z_sem.at[DZ.index(d)], {"z": mod(z + d, NZ)}).start()

    def panel_of(k, low):
        return mod(z - DZ[k], NZ) * 2 + low

    def spread_y(k, part, turn):
        ref = kv.at[piece(panel_of(k, ylo), c, part)]
        to = {"ylo": 1 - ylo, "yhi": mod(yhi + ylo - lax.rem(part, 2), NY)}
        remote(ref, ref, send_sem.at[0], y_sem.at[k, turn], to).start()

    def spread_core(panel, part, slot):
        ref = kv.at[piece(panel, c, part)]
        remote(ref, ref, send_sem.at[0], c_sem.at[slot], partner).start()

    def spread_x(k, part, turn, step):
        ref = kv.at[piece(panel_of(k, ylo), c, part)]
        remote(ref, ref, send_sem.at[0], x_sem.at[k, turn], {"x": mod(x + step, NX)}).start()

    parts = (x, mod(x - way, NX), mod(x + way, NX), mod(x + 2, NX))

    def stage_z(k):
        if k:
            arrived(kv.at[piece(panel_of(k, ylo), c, x)], z_sem.at[k])
            spread_x(k, x, 0, way)
            spread_x(k, x, 1, -way)
        spread_y(k, x, 0)
        if k:
            spread_core(panel_of(k, ylo), x, k)

    def stage_x(k, turns):
        for turn in turns:
            part = parts[turn + 1]
            if k:
                arrived(kv.at[piece(panel_of(k, ylo), c, part)], x_sem.at[k, turn])
            if k and turn == 0:
                spread_x(k, part, 2, way)
            spread_y(k, part, turn + 1)
            if k:
                spread_core(panel_of(k, ylo), part, k)

    def stage_y(k):
        panel = panel_of(k, 1 - ylo)
        for turn in range(4):
            arrived(kv.at[piece(panel, c, parts[turn])], y_sem.at[k, turn])
            spread_core(panel, parts[turn], 8 + k)

    def stage_core(k):
        if k:
            arrived(kv.at[pl.ds(piece(panel_of(k, ylo), 1 - c, 0), 4)], c_sem.at[k])
        arrived(kv.at[pl.ds(piece(panel_of(k, 1 - ylo), 1 - c, 0), 4)], c_sem.at[8 + k])

    def share(quarter):
        ref = wide.at[pl.ds(pl.multiple_of(SLICE * ylo + 112 * quarter, 16), 112)]
        remote(ref, ref, send_sem.at[5], w_sem.at[quarter], {"ylo": 1 - ylo}).start()

    across = lax.broadcasted_iota(jnp.int32, (ROWS, ROWS), 1)
    down = lax.broadcasted_iota(jnp.int32, (ROWS, ROWS), 0)
    row_pos = jnp.sum(
        jnp.where(across == down, query_pos[...].astype(f32), 0.0), axis=1, keepdims=True
    )

    rows_pos = jnp.concatenate([row_pos] * (BLOCK // ROWS), axis=0)

    def absorb():
        for load in loads[10:13]:
            load.wait()
        for h in range(HEADS):
            lifted = jnp.dot(
                nope[:, NOPE * h : NOPE * h + NOPE], lift[h], preferred_element_type=f32
            )
            at = slice(ROWS * h, ROWS * h + ROWS)
            query[at, :LATENT] = lifted.astype(bf)
            query[at, LATENT:] = turned[:, ROPE * h : ROPE * h + ROPE]

    def attend(k):
        panels = (panel_of(k, ylo), panel_of(k, 1 - ylo))
        lane = lax.broadcasted_iota(jnp.int32, (1, 128), 1)
        spots = jnp.concatenate(
            [blocks[p] * PANEL + 128 * half + lane for p in panels for half in range(2)], axis=1
        ).astype(f32)

        def one_block(b, carry):
            at = pl.ds(pl.multiple_of(BLOCK * b, BLOCK), BLOCK)
            keys = jnp.concatenate(
                [
                    kv[pl.ds(piece(p, half, 0), 4)].reshape(KEYS, 128)
                    for p in panels
                    for half in range(2)
                ],
                axis=1,
            )
            scores = jnp.dot(query[at, :], keys, preferred_element_type=f32)
            scores = jnp.where(spots <= rows_pos, scores * softmax_scale, -jnp.inf)
            top = jnp.max(scores, axis=1, keepdims=True)
            if k:
                before = best[at, :1]
                top = jnp.maximum(before, top)
                shrink = jnp.exp(before - top)
            else:
                top = jnp.maximum(top, LOWEST)
            weights = jnp.exp(scores - top)
            total = jnp.sum(weights, axis=1, keepdims=True)
            update = lax.dot_general(
                weights.astype(bf), keys[:LATENT], (((1,), (1,)), ((), ())),
                preferred_element_type=f32,
            )
            if k:
                total = total + denom[at, :1] * shrink
                update = update + mixed[at, :] * shrink
            best[at, :] = jnp.broadcast_to(top, (BLOCK, 128))
            denom[at, :] = jnp.broadcast_to(total, (BLOCK, 128))
            mixed[at, :] = update
            return carry

        lax.fori_loop(0, HEADS * ROWS // BLOCK, one_block, 0)

    for t in range(NZ + SHIFTS[-1]):
        if t < NZ:
            stage_z(t)
        if t == 2:
            absorb()
            loads[14].wait()
        if 0 <= t - SHIFTS[0] < NZ:
            stage_x(t - SHIFTS[0], (0, 1))
        if 0 <= t - SHIFTS[1] < NZ:
            stage_x(t - SHIFTS[1], (2,))
        if t in SHARES:
            share(SHARES.index(t))
        if 0 <= t - SHIFTS[2] < NZ:
            stage_y(t - SHIFTS[2])
        if 0 <= t - SHIFTS[3] < NZ:
            stage_core(t - SHIFTS[3])
            attend(t - SHIFTS[3])

    steps = ({"z": mod(z + 1, NZ)}, {"z": mod(z - 1, NZ)})

    def publish(sub):
        for side in range(2):
            remote(
                vals.at[sub], vall.at[SUBS * z + sub], send_sem.at[1], ag_sem.at[side, 0, sub],
                steps[side],
            ).start()

    loads[13].wait()
    source = ((down % 64) // 4) * 8 + (down // 64) * 4 + down % 4
    order = jnp.where(across == source, 1.0, 0.0).astype(bf)
    for h in (0, 2, 1, 3):
        at = slice(ROWS * h, ROWS * h + ROWS)
        latent = (mixed[at, :] * (1.0 / denom[at, :1])).astype(bf)
        head = jnp.dot(latent, expand[h], preferred_element_type=f32).astype(bf)
        head = jnp.dot(order, head, preferred_element_type=f32).astype(bf)
        vals[h] = head
        publish(h)

    def land(dist):
        for sub in (0, 2, 1, 3):
            for side in range(2):
                if dist > LIMIT[side][sub]:
                    continue
                source = mod(z + (dist if side else -dist), NZ)
                ref = vall.at[SUBS * source + sub]
                arrived(ref, ag_sem.at[side, dist - 1, sub])
                if dist + 1 <= LIMIT[side][sub]:
                    remote(
                        ref, ref, send_sem.at[1], ag_sem.at[side, dist, sub], steps[side]
                    ).start()

    def multiply(m):
        held = [vall.at[SUBS * mod(z + OFF[m], NZ) + h] if m else vals.at[h] for h in range(HEADS)]
        rows = jnp.concatenate([ref[...] for ref in held], axis=1)
        product = lax.dot_general(
            rows, wide[...], (((1,), (1,)), ((), ())), preferred_element_type=f32
        )
        acc[m] = product.reshape(2, 64, 2 * SLICE)
        cs[m] = acc[m, 1 - c].astype(bf)
        remote(cs.at[m], cr.at[m], send_sem.at[2], d_sem.at[m], partner).start()

    def reduce_core(m):
        arrived(cr.at[m], d_sem.at[m])
        for d in (2, 1, 3, 0):
            at = pl.ds(pl.multiple_of(16 * mod(x + d, NX), 16), 16)
            both = acc[m, c, at, :] + cr[m, at, :].astype(f32)
            if d:
                xs[m, d - 1] = both.astype(bf)
            else:
                xown[m] = both
            if d:
                remote(
                    xs.at[m, d - 1], xr.at[m, d - 1], send_sem.at[3], r_sem.at[m, d - 1],
                    {"x": mod(x + d, NX)},
                ).start()

    def reduce_x(m):
        for d in range(3):
            arrived(xr.at[m, d], r_sem.at[m, d])
        total = xown[m]
        for d in range(3):
            total = total + xr[m, d].astype(f32)
        for y in range(NY):
            fs[NY * m + y] = total[4 * y : 4 * y + 4].astype(bf)
        for d in (2, 1, 3, 0):
            ref = fs.at[NY * m + mod(yhi + d, NY)]
            if m or d:
                remote(ref, fr.at[m, d], send_sem.at[4], f_sem.at[m, d], home(m, d)).start()
            else:
                fr[0, 0] = fs[yhi]

    for step in ORDER:
        if step == ("m", 0):
            for quarter in range(4):
                away = pl.multiple_of(SLICE * (1 - ylo) + 112 * quarter, 16)
                arrived(wide.at[pl.ds(away, 112)], w_sem.at[quarter])
        {"a": land, "m": multiply, "c": reduce_core, "x": reduce_x}[step[0]](step[1])
    for m in range(NZ):
        for d in range(NY):
            if m or d:
                arrived(fr.at[m, d], f_sem.at[m, d])
        total = fr[m, 0].astype(f32)
        for d in range(1, NY):
            total = total + fr[m, d].astype(f32)
        at = pl.multiple_of(2 * SLICE * mod(z - OFF[m], NZ), 2 * SLICE)
        out[:, pl.ds(at, 2 * SLICE)] = total.astype(bf)
    pieces = kv.at[pl.ds(0, 7 + 21 + 32 + 28 + 32)]
    sent = (pieces, vall.at[pl.ds(0, 7 * SUBS)], cs, xs, fs.at[pl.ds(0, 31)], wide.at[near])
    for i, ref in enumerate(sent):
        remote(ref, ref, send_sem.at[i], w_sem.at[0], partner).wait_send()


def attention(*operands):
    bf, f32 = jnp.bfloat16, jnp.float32
    anywhere = pl.BlockSpec(memory_space=pl.ANY)
    vmem = pl.BlockSpec(memory_space=pltpu.VMEM)
    smem = pl.BlockSpec(memory_space=pltpu.SMEM)
    return pl.pallas_call(
        kernel,
        out_shape=jax.ShapeDtypeStruct((4, NZ * 2 * SLICE), bf),
        in_specs=[anywhere] * 4 + [smem, vmem] + [anywhere] * 3,
        out_specs=vmem,
        scratch_shapes=[
            pltpu.VMEM((128, 144, 128), bf),
            pltpu.VMEM((ROWS, HEADS * NOPE), bf),
            pltpu.VMEM((ROWS, HEADS * ROPE), bf),
            pltpu.VMEM((HEADS, LATENT, VHEAD), bf),
            pltpu.VMEM((HEADS, NOPE, LATENT), bf),
            pltpu.VMEM((2 * SLICE, HEADS * VHEAD), bf),
            pltpu.VMEM((HEADS * ROWS, KEYS), bf),
            pltpu.VMEM((HEADS * ROWS, 128), f32),
            pltpu.VMEM((HEADS * ROWS, 128), f32),
            pltpu.VMEM((HEADS * ROWS, LATENT), f32),
            pltpu.VMEM((SUBS, ROWS, VHEAD), bf),
            pltpu.VMEM((NZ * SUBS, ROWS, VHEAD), bf),
            pltpu.VMEM((8, 2, 64, 2 * SLICE), f32),
            pltpu.VMEM((8, 64, 2 * SLICE), bf),
            pltpu.VMEM((8, 64, 2 * SLICE), bf),
            pltpu.VMEM((8, 3, 16, 2 * SLICE), bf),
            pltpu.VMEM((8, 3, 16, 2 * SLICE), bf),
            pltpu.VMEM((8, 16, 2 * SLICE), f32),
            pltpu.VMEM((32, 4, 2 * SLICE), bf),
            pltpu.VMEM((8, 4, 4, 2 * SLICE), bf),
            pltpu.SemaphoreType.DMA((15,)),
            pltpu.SemaphoreType.DMA((6,)),
            pltpu.SemaphoreType.DMA((8,)),
            pltpu.SemaphoreType.DMA((8, 3)),
            pltpu.SemaphoreType.DMA((8, 4)),
            pltpu.SemaphoreType.DMA((16,)),
            pltpu.SemaphoreType.DMA((4,)),
            pltpu.SemaphoreType.DMA((2, 4, SUBS)),
            pltpu.SemaphoreType.DMA((8,)),
            pltpu.SemaphoreType.DMA((8, 3)),
            pltpu.SemaphoreType.DMA((8, 4)),
        ],
        compiler_params=pltpu.CompilerParams(
            collective_id=0, has_side_effects=True, vmem_limit_bytes=56 << 20
        ),
        name="attention",
    )(*operands)


def on_device(q_nope, q_rope, latent_keys, rope_keys, panel_block, query_pos, w_uk, w_uv, w_out):
    return attention(
        q_nope, q_rope, latent_keys, rope_keys, panel_block, query_pos.reshape(1, ROWS),
        w_uk, w_uv, w_out,
    )


def solution(mesh):
    finer = Mesh(mesh.devices.reshape(NZ, 2, NX, NY, 2), AXES)
    return jax.shard_map(
        on_device,
        mesh=finer,
        in_specs=(
            P(ROW, HEAD),
            P(ROW, HEAD),
            P(None, ROW),
            P(None, ROW),
            P(),
            P(ROW),
            P(HEAD, None, None),
            P(HEAD, None, None),
            P(ROW, HEAD),
        ),
        out_specs=P(ROW + HEAD, None),
        check_vma=False,
    )
```
